128 devices in a mesh: high: 8 (over x, core), low: 16 (over z, y).
Axes of the slice: x: 4, y: 4, z: 4, core: 2. Of those that a mesh axis runs over, the one named last changes fastest.
Arguments:
- wave_parts: float32 [2, 2048, 128, 128], P(None, ('high', 'low')), may hold values from -6 to 6
- level_table: float32 [2048, 128, 128], P(('high', 'low')), may hold values from -2 to 2
- diagonal_angles: float32 [2, 128], replicated, may hold values from 0.3 to 1.2
- turn_angles: float32 [2, 4], replicated, may hold values from 0.3 to 1.2
Outputs:
- state_after: float32 [2, 2048, 128, 128], P(None, ('high', 'low'))
The draws below stay inside these ranges and needn't reach their ends.
All inputs are finite; a program needn't handle non-finite values.
Results may differ from the reference program's by a relative error of at most 0.0003.
Values sent between devices are 32-bit elements.
No kernel may reach another device: no remote copies, remote signals or barrier semaphores. Data moves between devices by JAX's collectives and lax.ppermute only.
A program may use at most 64 MiB of HBM per device.

```python
import jax
import jax.numpy as jnp
from jax import lax

BLOCKS_DEV = 16
ROWS = 128
LANES = 128
BLOCKS = 2048
LAYERS = 2
N_HIGH = 8
N_LOW = 16


def block_scale(key, shape, cuts, least, high):
    level = 1.0
    for axis_at, shards_of in cuts:
        heights = jax.random.uniform(jax.random.fold_in(jax.random.fold_in(key, 6), axis_at), (shards_of,), jnp.float32, least / len(cuts), high / len(cuts))
        level = level * jnp.repeat(jnp.exp(heights), shape[axis_at] // shards_of).reshape((-1,) + (1,) * (len(shape) - 1 - axis_at))
    return level


def scatter_about(own_key, shape, deviation, reach, shards=(), kind=jnp.bfloat16):
    level = block_scale(own_key, shape, shards, -0.22, 0.18) if shards else 1.0
    array = jax.random.normal(own_key, shape, jnp.float32) * deviation * level
    return jnp.minimum(jnp.maximum(array, -reach), reach).astype(kind)


def setup_inputs(seed: int = 0) -> dict:
    key_of = jax.random.split(jax.random.key(seed), 5)
    return {
        "wave_parts": scatter_about(key_of[0], (2, BLOCKS, ROWS, LANES), 1.0, 6.0, ((1, 128),), jnp.float32),
        "level_table": jnp.clip(jax.random.uniform(key_of[1], (BLOCKS, ROWS, LANES), jnp.float32, -2.0, 2.0) * block_scale(key_of[1], (BLOCKS, ROWS, LANES), ((0, 128),), -0.4, 0.0), -2.0, 2.0),
        "diagonal_angles": jnp.clip(jax.random.uniform(key_of[2], (LAYERS, LANES), jnp.float32, 0.3, 1.2), 0.3, 1.2),
        "turn_angles": jnp.clip(jax.random.uniform(key_of[3], (LAYERS, 4), jnp.float32, 0.3, 1.2), 0.3, 1.2),
    }


def count_bits(values, count):
    places = jnp.arange(count.bit_length() - 1, dtype=jnp.int32)
    return jnp.sum((values[..., None] >> places) & 1, axis=-1)


def mix_table(count, angle):
    rank = jnp.arange(count, dtype=jnp.int32)
    apart = count_bits(rank[:, None] ^ rank[None, :], count)
    bits = count.bit_length() - 1
    size = jnp.cos(angle) ** (bits - apart).astype(jnp.float32) * jnp.sin(angle) ** apart.astype(jnp.float32)
    real_sign = jnp.where(apart % 4 == 0, 1.0, jnp.where(apart % 4 == 2, -1.0, 0.0)).astype(jnp.float32)
    imag_sign = jnp.where(apart % 4 == 1, -1.0, jnp.where(apart % 4 == 3, 1.0, 0.0)).astype(jnp.float32)
    return size * real_sign, size * imag_sign


def turn_dim(values, dim, angle):
    real_part, imag_part = mix_table(values.shape[dim], angle)
    def times(table):
        moved = jnp.tensordot(values, table, axes=([dim], [0]), precision=lax.Precision.HIGHEST)
        return jnp.moveaxis(moved, -1, dim)
    by_real = times(real_part)
    by_imag = times(imag_part)
    return jnp.stack([by_real[0] - by_imag[1], by_real[1] + by_imag[0]])


def diagonal_step(values, levels, angle):
    turn = angle * levels
    return jnp.stack([values[0] * jnp.cos(turn) + values[1] * jnp.sin(turn), values[1] * jnp.cos(turn) - values[0] * jnp.sin(turn)])


def reference(wave_parts, level_table, diagonal_angles, turn_angles):
    values = wave_parts
    for layer in range(LAYERS):
        values = diagonal_step(values, level_table, diagonal_angles[layer])
        values = turn_dim(values, 3, turn_angles[layer, 0])
        values = turn_dim(values, 2, turn_angles[layer, 1])
        parts = values.reshape(2, N_HIGH, N_LOW, BLOCKS_DEV, ROWS, LANES)
        parts = turn_dim(parts, 1, turn_angles[layer, 2])
        parts = turn_dim(parts, 2, turn_angles[layer, 3])
        parts = turn_dim(parts, 3, turn_angles[layer, 2])
        values = parts.reshape(values.shape)
    return values
```

```python
import jax
import jax.numpy as jnp
from jax import lax
from jax.experimental import pallas as pl
from jax.experimental.pallas import tpu as pltpu
from jax.sharding import PartitionSpec as P

HIGH_LOW = ("high", "low")
DEVICES = 128
BLOCKS = 16
ROWS = 128
LANES = 128
CHUNK = 16
F32 = jnp.float32
BF16 = jnp.bfloat16

COS = (0.9999999403953552, -0.4999995529651642, 0.04166578873991966,
       -0.0013882378116250038, 2.4582879632362165e-05, -2.4136278398145805e-07)
SIN = (1.0, -0.16666662693023682, 0.008333264850080013,
       -0.0001983620022656396, 2.7387263799028005e-06, -2.2399454735477775e-08)


def poly(coefficients, z):
    total = coefficients[-1] * z + coefficients[-2]
    for c in coefficients[-3::-1]:
        total = total * z + c
    return total


def cos_sin(x):
    z = x * x
    return poly(COS, z), x * poly(SIN, z)


def angle_parts(turn_ref, layer):
    return [cos_sin(jnp.full((1, LANES), turn_ref[layer, g], F32)) for g in range(4)]


def power(x, n):
    total = x
    for _ in range(n - 1):
        total = total * x
    return total


def rotation(parts, scale, transposed):
    row = lax.broadcasted_iota(jnp.int32, (128, 128), 0)
    col = lax.broadcasted_iota(jnp.int32, (128, 128), 1)
    out, come = (col, row) if transposed else (row, col)
    total = jnp.broadcast_to(scale, (128, 128))
    for k, (c, s) in enumerate(parts):
        place = 1 << (6 - k)
        same = ((out ^ come) & place) == 0
        signed = jnp.where((out & place) != 0, -s, s)
        total = total * jnp.where(same, c, signed)
    return total


def split(x):
    top = x.astype(BF16)
    return top, (x - top.astype(F32)).astype(BF16)


def left_matrix(parts, scale):
    top, rest = split(rotation(parts, scale, False))
    zero = jnp.zeros_like(top)
    return jnp.concatenate(
        [jnp.concatenate([top, top], 1), jnp.concatenate([rest, zero], 1)], 0
    )


def right_matrix(parts, scale):
    top, rest = split(rotation(parts, scale, True))
    zero = jnp.zeros_like(top)
    return jnp.concatenate(
        [jnp.concatenate([top, rest], 1), jnp.concatenate([top, zero], 1)], 0
    )


def mix_rows_lanes(re, im, left, right):
    re_top, re_rest = split(re)
    im_top, im_rest = split(im)
    block = jnp.concatenate(
        [jnp.concatenate([re_top, im_top], 1), jnp.concatenate([re_rest, im_rest], 1)], 0
    )
    both = jnp.dot(left, block, preferred_element_type=F32)
    both = both[:128] + both[128:]
    re_top, re_rest = split(both[:, :128])
    im_top, im_rest = split(both[:, 128:])
    block = jnp.concatenate(
        [jnp.concatenate([re_top, re_rest], 1), jnp.concatenate([im_top, im_rest], 1)], 0
    )
    both = jnp.dot(block, right, preferred_element_type=F32)
    both = both[:, :128] + both[:, 128:]
    return both[:128], both[128:]


def butterflies(values, tangents):
    values = list(values)
    for k, t in enumerate(tangents):
        apart = len(values) >> (k + 1)
        for i in range(len(values)):
            if not i & apart:
                u, v = values[i], values[i + apart]
                values[i], values[i + apart] = u + t * v, v - t * u
    return values


def count_bits(x, bits):
    total = x & 1
    for k in range(1, bits):
        total = total + ((x >> k) & 1)
    return total


def device_bits():
    return count_bits(lax.axis_index("high"), 3) + count_bits(lax.axis_index("low"), 4)


def set_phases(odd_ref, re_sign_ref, im_sign_ref, rows, low_rows, back):
    row = lax.broadcasted_iota(jnp.int32, (rows, LANES), 0)
    lane = lax.broadcasted_iota(jnp.int32, (rows, LANES), 1)
    bits = count_bits(row, low_rows) + count_bits(lane, 7)
    for k in range(4):
        p = (bits + k) & 3
        odd_ref[k] = (p & 1).astype(F32)
        plus, minus = (1 - (p & 2)).astype(F32), (1 - ((p + 1) & 2)).astype(F32)
        re_sign_ref[k] = minus if back else plus
        im_sign_ref[k] = plus if back else minus


def first_kernel(turn_ref, angle_ref, wave_ref, level_ref, out_ref, wave, left, right,
                 odd, re_sign, im_sign, wave_sem, level_sem):
    steps = 8
    per = BLOCKS // steps

    def wave_copy(i):
        return pltpu.make_async_copy(
            wave_ref.at[:, pl.ds(i * per, per)], wave.at[i], wave_sem.at[i]
        )

    def level_copy(i):
        return pltpu.make_async_copy(
            level_ref.at[pl.ds(i * per * 8, per * 8)],
            out_ref.at[pl.ds(i * per * 8, per * 8), pl.ds(2 * CHUNK, CHUNK)],
            level_sem.at[i],
        )

    for i in range(steps):
        level_copy(i).start()
        wave_copy(i).start()

    parts = angle_parts(turn_ref, 0)
    (c0, s0), (c1, s1), (c2, s2), (c3, s3) = parts
    left[...] = left_matrix([parts[1]] * 7, jnp.ones_like(c1))
    right[...] = right_matrix([parts[0]] * 7, power(c2, 7) * power(c3, 4))
    set_phases(odd, re_sign, im_sign, ROWS, 7, False)
    angle = angle_ref[0:1]
    elsewhere = device_bits()

    @pl.loop(0, steps)
    def _(i):
        level_copy(i).wait()
        wave_copy(i).wait()
        for j in range(per):
            b = i * per + j
            k = (elsewhere + count_bits(b, 4)) & 3
            level = out_ref[pl.ds(b * 8, 8), pl.ds(2 * CHUNK, CHUNK)].reshape(ROWS, LANES)
            co, si = cos_sin(level * angle)
            re, im = wave[i, 0, j], wave[i, 1, j]
            swap = odd[k] > 0.5
            u = jnp.where(swap, im, re) * re_sign[k]
            v = jnp.where(swap, re, im) * im_sign[k]
            re, im = mix_rows_lanes(u * co + v * si, v * co - u * si, left[...], right[...])
            out_ref[pl.ds(b * 8, 8), pl.ds(0, CHUNK)] = re.reshape(8, CHUNK, LANES)
            out_ref[pl.ds(b * 8, 8), pl.ds(CHUNK, CHUNK)] = im.reshape(8, CHUNK, LANES)

    t2 = jnp.broadcast_to(s2 / c2, (8, LANES))

    @pl.loop(0, 32)
    def _(i):
        at, tile = i // 4, pl.ds(pl.multiple_of((i % 4) * 8, 8), 8)
        values = [out_ref[b * 8 + at, tile] for b in range(BLOCKS)]
        for b, value in enumerate(butterflies(values, [t2] * 4)):
            out_ref[b * 8 + at, tile] = value


def middle_kernel(turn_ref, angle_ref, in_ref, out_ref, held, left, right):
    before, after = angle_parts(turn_ref, 0), angle_parts(turn_ref, 1)
    (c0, s0), (c1, s1), (c2, s2), (c3, s3) = after
    left[...] = left_matrix([after[3]] * 3 + [after[1]] * 4, jnp.ones_like(c1))
    right[...] = right_matrix([after[0]] * 7, power(c2, 7) * c3 * power(c1, 3))
    angle = jnp.broadcast_to(angle_ref[1:2], (8, LANES))
    t2, t3 = (jnp.broadcast_to(before[g][1] / before[g][0], (8, LANES)) for g in (2, 3))

    @pl.loop(0, 32)
    def _(i):
        at, tile = i // 4, pl.ds(pl.multiple_of((i % 4) * 8, 8), 8)
        values = [in_ref[at * 16 + low, tile] for low in range(16)]
        for low, value in enumerate(butterflies(values, [t3] * 4)):
            held[at * 16 + low, tile] = value

    @pl.loop(0, 32)
    def _(i):
        low, row = i // 2, pl.multiple_of((i % 2) * 8, 8)
        re = butterflies([held[h * 16 + low, pl.ds(row, 8)] for h in range(8)], [t2] * 3)
        im = butterflies([held[h * 16 + low, pl.ds(CHUNK + row, 8)] for h in range(8)], [t2] * 3)
        for h in range(8):
            co, si = cos_sin(in_ref[h * 16 + low, pl.ds(2 * CHUNK + row, 8)] * angle)
            held[h * 16 + low, pl.ds(row, 8)] = re[h] * co + im[h] * si
            held[h * 16 + low, pl.ds(CHUNK + row, 8)] = im[h] * co - re[h] * si

    @pl.loop(0, 8)
    def _(i):
        for j in range(2):
            at = pl.ds((i * 2 + j) * 8, 8)
            re = held[at, pl.ds(0, CHUNK)].reshape(128, LANES)
            im = held[at, pl.ds(CHUNK, CHUNK)].reshape(128, LANES)
            re, im = mix_rows_lanes(re, im, left[...], right[...])
            held[at, pl.ds(0, CHUNK)] = re.reshape(8, CHUNK, LANES)
            held[at, pl.ds(CHUNK, CHUNK)] = im.reshape(8, CHUNK, LANES)

    u2, u3 = (jnp.broadcast_to(after[g][1] / after[g][0], (8, LANES)) for g in (2, 3))

    @pl.loop(0, 32)
    def _(i):
        at, tile = i // 4, pl.ds(pl.multiple_of((i % 4) * 8, 8), 8)
        values = [held[k * 8 + at, tile] for k in range(16)]
        for k, value in enumerate(butterflies(values, [u2] * 3 + [u3])):
            out_ref[k * 8 + at, tile] = value


def last_kernel(turn_ref, in_ref, out_ref, held, done, odd, re_sign, im_sign, sem):
    parts = angle_parts(turn_ref, 1)
    t1, t2 = (jnp.broadcast_to(parts[g][1] / parts[g][0], (8, LANES)) for g in (1, 2))
    set_phases(odd, re_sign, im_sign, CHUNK, 4, True)
    elsewhere = device_bits()

    @pl.loop(0, 32)
    def _(i):
        at, tile = i // 4, pl.ds(pl.multiple_of((i % 4) * 8, 8), 8)
        values = [in_ref[b * 8 + at, tile] for b in range(BLOCKS)]
        for b, value in enumerate(butterflies(values, [t2] * 4)):
            held[b * 8 + at, tile] = value

    def out_copy(b):
        return pltpu.make_async_copy(done.at[:, b], out_ref.at[:, b], sem.at[b])

    @pl.loop(0, BLOCKS)
    def _(b):
        base = elsewhere + count_bits(b, 4)
        for row in (0, 8):
            re = butterflies([held[b * 8 + r, pl.ds(row, 8)] for r in range(8)], [t1] * 3)
            im = butterflies([held[b * 8 + r, pl.ds(CHUNK + row, 8)] for r in range(8)], [t1] * 3)
            for r in range(8):
                k = (base + r.bit_count()) & 3
                swap = odd[k, pl.ds(row, 8)] > 0.5
                to = pl.ds(r * CHUNK + row, 8)
                done[0, b, to] = jnp.where(swap, im[r], re[r]) * re_sign[k, pl.ds(row, 8)]
                done[1, b, to] = jnp.where(swap, re[r], im[r]) * im_sign[k, pl.ds(row, 8)]
        out_copy(b).start()

    @pl.loop(0, BLOCKS)
    def _(b):
        out_copy(b).wait()


LIMIT = pltpu.CompilerParams(vmem_limit_bytes=20 << 20)


def spec(space):
    return pl.BlockSpec(memory_space=space)


def on_device(wave_parts, level_table, diagonal_angles, turn_angles):
    smem, vmem, hbm = spec(pltpu.SMEM), spec(pltpu.VMEM), spec(pltpu.HBM)
    phases = [pltpu.VMEM((4, ROWS, LANES), F32)] * 3
    sent = pl.pallas_call(
        first_kernel,
        name="first",
        compiler_params=LIMIT,
        out_shape=jax.ShapeDtypeStruct((DEVICES, 3 * CHUNK, LANES), F32),
        in_specs=[smem, vmem, hbm, hbm],
        out_specs=vmem,
        scratch_shapes=[
            pltpu.VMEM((8, 2, 2, ROWS, LANES), F32),
            pltpu.VMEM((256, 256), BF16),
            pltpu.VMEM((256, 256), BF16),
            *phases,
            pltpu.SemaphoreType.DMA((8,)),
            pltpu.SemaphoreType.DMA((8,)),
        ],
    )(turn_angles, diagonal_angles, wave_parts, level_table.reshape(DEVICES, CHUNK, LANES))
    held = lax.all_to_all(sent, HIGH_LOW, 0, 0, tiled=True)
    sent = pl.pallas_call(
        middle_kernel,
        name="middle",
        compiler_params=LIMIT,
        out_shape=jax.ShapeDtypeStruct((DEVICES, 2 * CHUNK, LANES), F32),
        in_specs=[smem, vmem, vmem],
        out_specs=vmem,
        scratch_shapes=[
            pltpu.VMEM((DEVICES, 2 * CHUNK, LANES), F32),
            pltpu.VMEM((256, 256), BF16),
            pltpu.VMEM((256, 256), BF16),
        ],
    )(turn_angles, diagonal_angles, held)
    held = lax.all_to_all(sent, HIGH_LOW, 0, 0, tiled=True)
    phases = [pltpu.VMEM((4, CHUNK, LANES), F32)] * 3
    return pl.pallas_call(
        last_kernel,
        name="last",
        compiler_params=LIMIT,
        out_shape=jax.ShapeDtypeStruct((2, BLOCKS, ROWS, LANES), F32),
        in_specs=[smem, vmem],
        out_specs=hbm,
        scratch_shapes=[
            pltpu.VMEM((DEVICES, 2 * CHUNK, LANES), F32),
            pltpu.VMEM((2, BLOCKS, ROWS, LANES), F32),
            *phases,
            pltpu.SemaphoreType.DMA((BLOCKS,)),
        ],
    )(turn_angles, held)


def solution(mesh):
    placed = (P(None, HIGH_LOW, None, None), P(HIGH_LOW, None, None), P(), P())
    return jax.shard_map(
        on_device,
        mesh=mesh,
        in_specs=placed,
        out_specs=P(None, HIGH_LOW, None, None),
        check_vma=False,
    )
```

```python
import jax
import jax.numpy as jnp
from jax import lax
from jax.experimental import pallas as pl
from jax.experimental.pallas import tpu as pltpu
from jax.sharding import PartitionSpec as P

HIGH_LOW = ("high", "low")
DEVICES = 128
BLOCKS = 16
ROWS = 128
LANES = 128
LOWS = 8
STEPS = 2
CHUNK = 16
F32 = jnp.float32
BF16 = jnp.bfloat16

COS = (0.9999999403953552, -0.4999995529651642, 0.04166578873991966,
       -0.0013882378116250038, 2.4582879632362165e-05, -2.4136278398145805e-07)
SIN = (1.0, -0.16666662693023682, 0.008333264850080013,
       -0.0001983620022656396, 2.7387263799028005e-06, -2.2399454735477775e-08)


def poly(coefficients, z):
    total = coefficients[-1] * z + coefficients[-2]
    for c in coefficients[-3::-1]:
        total = total * z + c
    return total


def cos_sin(x):
    z = x * x
    return poly(COS, z), x * poly(SIN, z)


def angle_parts(turn_ref, layer):
    return [cos_sin(jnp.full((1, LANES), turn_ref[layer, g], F32)) for g in range(4)]


def power(x, n):
    total = x
    for _ in range(n - 1):
        total = total * x
    return total


def rotation(parts, scale, transposed):
    row = lax.broadcasted_iota(jnp.int32, (128, 128), 0)
    col = lax.broadcasted_iota(jnp.int32, (128, 128), 1)
    out, come = (col, row) if transposed else (row, col)
    total = jnp.broadcast_to(scale, (128, 128))
    for k, (c, s) in enumerate(parts):
        place = 1 << (6 - k)
        same = ((out ^ come) & place) == 0
        signed = jnp.where((out & place) != 0, -s, s)
        total = total * jnp.where(same, c, signed)
    return total


def split(x):
    top = x.astype(BF16)
    return top, (x - top.astype(F32)).astype(BF16)


def left_matrix(parts, scale):
    top, rest = split(rotation(parts, scale, False))
    zero = jnp.zeros_like(top)
    return jnp.concatenate(
        [jnp.concatenate([top, top], 1), jnp.concatenate([rest, zero], 1)], 0
    )


def right_matrix(parts, scale):
    top, rest = split(rotation(parts, scale, True))
    zero = jnp.zeros_like(top)
    return jnp.concatenate(
        [jnp.concatenate([top, rest], 1), jnp.concatenate([top, zero], 1)], 0
    )


def mix_rows_lanes(re, im, left, right):
    re_top, re_rest = split(re)
    im_top, im_rest = split(im)
    block = jnp.concatenate(
        [jnp.concatenate([re_top, im_top], 1), jnp.concatenate([re_rest, im_rest], 1)], 0
    )
    both = jnp.dot(left, block, preferred_element_type=F32)
    both = both[:128] + both[128:]
    re_top, re_rest = split(both[:, :128])
    im_top, im_rest = split(both[:, 128:])
    block = jnp.concatenate(
        [jnp.concatenate([re_top, re_rest], 1), jnp.concatenate([im_top, im_rest], 1)], 0
    )
    both = jnp.dot(block, right, preferred_element_type=F32)
    both = both[:, :128] + both[:, 128:]
    return both[:128], both[128:]


def butterflies(values, tangents):
    values = list(values)
    for k, t in enumerate(tangents):
        apart = len(values) >> (k + 1)
        for i in range(len(values)):
            if not i & apart:
                u, v = values[i], values[i + apart]
                values[i], values[i + apart] = u + t * v, v - t * u
    return values


def count_bits(x, bits):
    total = x & 1
    for k in range(1, bits):
        total = total + ((x >> k) & 1)
    return total


def mix_major(take, put, place, tangents):
    @pl.loop(0, 16)
    def _(i):
        at = i // 2
        for j in range(2):
            tile = pl.ds(pl.multiple_of((i % 2) * 16, 16) + j * 8, 8)
            values = [take[place(k, at), tile] for k in range(16)]
            for k, value in enumerate(butterflies(values, tangents)):
                put[place(k, at), tile] = value


def device_bits():
    return count_bits(lax.axis_index("high"), 3) + count_bits(lax.axis_index("low"), 4)


def set_phases(odd_ref, re_sign_ref, im_sign_ref, rows, low_rows, back):
    row = lax.broadcasted_iota(jnp.int32, (rows, LANES), 0)
    lane = lax.broadcasted_iota(jnp.int32, (rows, LANES), 1)
    bits = count_bits(row, low_rows) + count_bits(lane, 7)
    for k in range(4):
        p = (bits + k) & 3
        odd_ref[k] = (p & 1).astype(F32)
        plus, minus = (1 - (p & 2)).astype(F32), (1 - ((p + 1) & 2)).astype(F32)
        re_sign_ref[k] = minus if back else plus
        im_sign_ref[k] = plus if back else minus


def first_kernel(turn_hbm, angle_hbm, wave_ref, level_ref, out_ref, turn_ref, angle_ref, wave, left, right,
                 odd, re_sign, im_sign, small_sem, wave_sem, level_sem):
    steps = STEPS
    per = BLOCKS // steps

    def wave_copy(i):
        return pltpu.make_async_copy(
            wave_ref.at[:, pl.ds(i * per, per)], wave.at[i], wave_sem.at[i]
        )

    def level_copy(i):
        return pltpu.make_async_copy(
            level_ref.at[pl.ds(i * per * 8, per * 8)],
            out_ref.at[pl.ds(i * per * 8, per * 8), pl.ds(2 * CHUNK, CHUNK)],
            level_sem.at[i],
        )

    turn_copy = pltpu.make_async_copy(turn_hbm, turn_ref, small_sem.at[0])
    angle_copy = pltpu.make_async_copy(angle_hbm, angle_ref, small_sem.at[1])
    turn_copy.start()
    angle_copy.start()
    for i in range(steps):
        level_copy(i).start()
        wave_copy(i).start()

    set_phases(odd, re_sign, im_sign, ROWS, 7, False)
    turn_copy.wait()
    angle_copy.wait()
    parts = angle_parts(turn_ref, 0)
    (c0, s0), (c1, s1), (c2, s2), (c3, s3) = parts
    left[...] = left_matrix([parts[1]] * 7, jnp.ones_like(c1))
    right[...] = right_matrix([parts[0]] * 7, power(c2, 7) * power(c3, 4))
    angle = angle_ref[0:1]
    elsewhere = device_bits()

    @pl.loop(0, steps)
    def _(i):
        level_copy(i).wait()
        wave_copy(i).wait()
        for j in range(per):
            b = i * per + j
            k = (elsewhere + count_bits(b, 4)) & 3
            level = out_ref[pl.ds(b * 8, 8), pl.ds(2 * CHUNK, CHUNK)].reshape(ROWS, LANES)
            co, si = cos_sin(level * angle)
            re, im = wave[i, 0, j], wave[i, 1, j]
            swap = odd[k] > 0.5
            u = jnp.where(swap, im, re) * re_sign[k]
            v = jnp.where(swap, re, im) * im_sign[k]
            re, im = mix_rows_lanes(u * co + v * si, v * co - u * si, left[...], right[...])
            out_ref[pl.ds(b * 8, 8), pl.ds(0, CHUNK)] = re.reshape(8, CHUNK, LANES)
            out_ref[pl.ds(b * 8, 8), pl.ds(CHUNK, CHUNK)] = im.reshape(8, CHUNK, LANES)

    t2 = jnp.broadcast_to(s2 / c2, (8, LANES))

    mix_major(out_ref, out_ref, lambda k, at: k * 8 + at, [t2] * 4)


def middle_kernel(turn_ref, angle_ref, in_ref, out_ref, held, left, right):
    before, after = angle_parts(turn_ref, 0), angle_parts(turn_ref, 1)
    (c0, s0), (c1, s1), (c2, s2), (c3, s3) = after
    left[...] = left_matrix([after[2]] * 3 + [after[1]] * 4, jnp.ones_like(c1))
    right[...] = right_matrix([after[0]] * 7, power(c3, 4) * power(c2, 4) * power(c1, 3))
    angle = angle_ref[1:2]
    t2, t3 = (before[g][1] / before[g][0] for g in (2, 3))

    mix_major(in_ref, held, lambda k, at: at * 16 + k, [jnp.broadcast_to(t3, (8, LANES))] * 4)

    @pl.loop(0, 16 // LOWS)
    def _(i):
        for j in range(LOWS):
            low = i * LOWS + j
            at = [h * 16 + low for h in range(8)]
            re = butterflies([held[k, pl.ds(0, CHUNK)] for k in at], [t2] * 3)
            im = butterflies([held[k, pl.ds(CHUNK, CHUNK)] for k in at], [t2] * 3)
            turned = []
            for h in range(8):
                co, si = cos_sin(in_ref[at[h], pl.ds(2 * CHUNK, CHUNK)] * angle)
                turned.append((re[h] * co + im[h] * si, im[h] * co - re[h] * si))
            re, im = (jnp.concatenate(part, 0) for part in zip(*turned))
            re, im = mix_rows_lanes(re, im, left[...], right[...])
            for h in range(8):
                held[at[h], pl.ds(0, CHUNK)] = re[h * CHUNK : (h + 1) * CHUNK]
                held[at[h], pl.ds(CHUNK, CHUNK)] = im[h * CHUNK : (h + 1) * CHUNK]

    u3 = jnp.broadcast_to(s3 / c3, (8, LANES))
    mix_major(held, out_ref, lambda k, at: at * 16 + k, [u3] * 4)


def last_kernel(turn_ref, in_ref, out_ref, held, done, odd, re_sign, im_sign, sem):
    parts = angle_parts(turn_ref, 1)
    t1, t2 = (jnp.broadcast_to(parts[g][1] / parts[g][0], (8, LANES)) for g in (1, 2))
    set_phases(odd, re_sign, im_sign, CHUNK, 4, True)
    elsewhere = device_bits()

    mix_major(in_ref, held, lambda k, at: k * 8 + at, [t2] * 4)

    def out_copy(b):
        return pltpu.make_async_copy(done.at[:, b], out_ref.at[:, b], sem.at[b])

    @pl.loop(0, BLOCKS)
    def _(b):
        base = elsewhere + count_bits(b, 4)
        for row in (0, 8):
            re = butterflies([held[b * 8 + r, pl.ds(row, 8)] for r in range(8)], [t1] * 3)
            im = butterflies([held[b * 8 + r, pl.ds(CHUNK + row, 8)] for r in range(8)], [t1] * 3)
            for r in range(8):
                k = (base + r.bit_count()) & 3
                swap = odd[k, pl.ds(row, 8)] > 0.5
                to = pl.ds(r * CHUNK + row, 8)
                done[0, b, to] = jnp.where(swap, im[r], re[r]) * re_sign[k, pl.ds(row, 8)]
                done[1, b, to] = jnp.where(swap, re[r], im[r]) * im_sign[k, pl.ds(row, 8)]
        out_copy(b).start()

    @pl.loop(0, BLOCKS)
    def _(b):
        out_copy(b).wait()


LIMIT = pltpu.CompilerParams(vmem_limit_bytes=20 << 20)


def spec(space):
    return pl.BlockSpec(memory_space=space)


def on_device(wave_parts, level_table, diagonal_angles, turn_angles):
    smem, vmem, hbm = spec(pltpu.SMEM), spec(pltpu.VMEM), spec(pltpu.HBM)
    phases = [pltpu.VMEM((4, ROWS, LANES), F32)] * 3
    sent = pl.pallas_call(
        first_kernel,
        name="first",
        compiler_params=LIMIT,
        out_shape=jax.ShapeDtypeStruct((DEVICES, 3 * CHUNK, LANES), F32),
        in_specs=[hbm] * 4,
        out_specs=vmem,
        scratch_shapes=[
            pltpu.SMEM((2, 4), F32),
            pltpu.VMEM((2, LANES), F32),
            pltpu.VMEM((STEPS, 2, BLOCKS // STEPS, ROWS, LANES), F32),
            pltpu.VMEM((256, 256), BF16),
            pltpu.VMEM((256, 256), BF16),
            *phases,
            pltpu.SemaphoreType.DMA((2,)),
            pltpu.SemaphoreType.DMA((STEPS,)),
            pltpu.SemaphoreType.DMA((STEPS,)),
        ],
    )(
        *(
            pltpu.with_memory_space_constraint(x, pltpu.HBM)
            for x in (
                turn_angles,
                diagonal_angles,
                wave_parts,
                level_table.reshape(DEVICES, CHUNK, LANES),
            )
        )
    )
    held = lax.all_to_all(sent, HIGH_LOW, 0, 0, tiled=True)
    sent = pl.pallas_call(
        middle_kernel,
        name="middle",
        compiler_params=LIMIT,
        out_shape=jax.ShapeDtypeStruct((DEVICES, 2 * CHUNK, LANES), F32),
        in_specs=[smem, vmem, vmem],
        out_specs=vmem,
        scratch_shapes=[
            pltpu.VMEM((DEVICES, 2 * CHUNK, LANES), F32),
            pltpu.VMEM((256, 256), BF16),
            pltpu.VMEM((256, 256), BF16),
        ],
    )(turn_angles, diagonal_angles, held)
    held = lax.all_to_all(sent, HIGH_LOW, 0, 0, tiled=True)
    phases = [pltpu.VMEM((4, CHUNK, LANES), F32)] * 3
    return pl.pallas_call(
        last_kernel,
        name="last",
        compiler_params=LIMIT,
        out_shape=jax.ShapeDtypeStruct((2, BLOCKS, ROWS, LANES), F32),
        in_specs=[smem, vmem],
        out_specs=hbm,
        scratch_shapes=[
            pltpu.VMEM((DEVICES, 2 * CHUNK, LANES), F32),
            pltpu.VMEM((2, BLOCKS, ROWS, LANES), F32),
            *phases,
            pltpu.SemaphoreType.DMA((BLOCKS,)),
        ],
    )(turn_angles, held)


def solution(mesh):
    placed = (P(None, HIGH_LOW, None, None), P(HIGH_LOW, None, None), P(), P())
    return jax.shard_map(
        on_device,
        mesh=mesh,
        in_specs=placed,
        out_specs=P(None, HIGH_LOW, None, None),
        check_vma=False,
    )
```

```python
import jax
import jax.numpy as jnp
from jax import lax
from jax.experimental import pallas as pl
from jax.experimental.pallas import tpu as pltpu
from jax.sharding import PartitionSpec as P

HIGH_LOW = ("high", "low")
DEVICES = 128
BLOCKS = 16
ROWS = 128
LANES = 128
LOWS = 16
STEPS = 2
CHUNK = 16
F32 = jnp.float32
BF16 = jnp.bfloat16

COS = (0.9999999403953552, -0.4999995529651642, 0.04166578873991966,
       -0.0013882378116250038, 2.4582879632362165e-05, -2.4136278398145805e-07)
SIN = (1.0, -0.16666662693023682, 0.008333264850080013,
       -0.0001983620022656396, 2.7387263799028005e-06, -2.2399454735477775e-08)


def poly(coefficients, z):
    total = coefficients[-1] * z + coefficients[-2]
    for c in coefficients[-3::-1]:
        total = total * z + c
    return total


def cos_sin(x):
    z = x * x
    return poly(COS, z), x * poly(SIN, z)


def angle_parts(turn_ref, layer):
    return [cos_sin(jnp.full((1, LANES), turn_ref[layer, g], F32)) for g in range(4)]


def power(x, n):
    total = x
    for _ in range(n - 1):
        total = total * x
    return total


def rotation(parts, scale, transposed):
    row = lax.broadcasted_iota(jnp.int32, (128, 128), 0)
    col = lax.broadcasted_iota(jnp.int32, (128, 128), 1)
    out, come = (col, row) if transposed else (row, col)
    total = jnp.broadcast_to(scale, (128, 128))
    for k, (c, s) in enumerate(parts):
        place = 1 << (6 - k)
        same = ((out ^ come) & place) == 0
        signed = jnp.where((out & place) != 0, -s, s)
        total = total * jnp.where(same, c, signed)
    return total


def split(x):
    top = x.astype(BF16)
    return top, (x - top.astype(F32)).astype(BF16)


def left_matrix(parts, scale):
    top, rest = split(rotation(parts, scale, False))
    zero = jnp.zeros_like(top)
    return jnp.concatenate(
        [jnp.concatenate([top, top], 1), jnp.concatenate([rest, zero], 1)], 0
    )


def right_matrix(parts, scale):
    top, rest = split(rotation(parts, scale, True))
    zero = jnp.zeros_like(top)
    return jnp.concatenate(
        [jnp.concatenate([top, rest], 1), jnp.concatenate([top, zero], 1)], 0
    )


def mix_rows_lanes(re, im, left, right):
    re_top, re_rest = split(re)
    im_top, im_rest = split(im)
    block = jnp.concatenate(
        [jnp.concatenate([re_top, im_top], 1), jnp.concatenate([re_rest, im_rest], 1)], 0
    )
    both = jnp.dot(left, block, preferred_element_type=F32)
    both = both[:128] + both[128:]
    re_top, re_rest = split(both[:, :128])
    im_top, im_rest = split(both[:, 128:])
    block = jnp.concatenate(
        [jnp.concatenate([re_top, re_rest], 1), jnp.concatenate([im_top, im_rest], 1)], 0
    )
    both = jnp.dot(block, right, preferred_element_type=F32)
    both = both[:, :128] + both[:, 128:]
    return both[:128], both[128:]


def butterflies(values, tangents):
    values = list(values)
    for k, t in enumerate(tangents):
        apart = len(values) >> (k + 1)
        for i in range(len(values)):
            if not i & apart:
                u, v = values[i], values[i + apart]
                values[i], values[i + apart] = u + t * v, v - t * u
    return values


def count_bits(x, bits):
    total = x & 1
    for k in range(1, bits):
        total = total + ((x >> k) & 1)
    return total


def mix_major(take, put, place, tangents):
    @pl.loop(0, 8)
    def _(at):
        for row in range(0, 32, 8):
            tile = pl.ds(row, 8)
            values = [take[place(k, at), tile] for k in range(16)]
            for k, value in enumerate(butterflies(values, tangents)):
                put[place(k, at), tile] = value


def device_bits():
    return count_bits(lax.axis_index("high"), 3) + count_bits(lax.axis_index("low"), 4)


def set_phases(odd_ref, re_sign_ref, im_sign_ref, rows, low_rows, back):
    row = lax.broadcasted_iota(jnp.int32, (rows, LANES), 0)
    lane = lax.broadcasted_iota(jnp.int32, (rows, LANES), 1)
    bits = count_bits(row, low_rows) + count_bits(lane, 7)
    for k in range(4):
        p = (bits + k) & 3
        odd_ref[k] = (p & 1).astype(F32)
        plus, minus = (1 - (p & 2)).astype(F32), (1 - ((p + 1) & 2)).astype(F32)
        re_sign_ref[k] = minus if back else plus
        im_sign_ref[k] = plus if back else minus


def later_tables(before, after, angle_ref, left, right, rows):
    (c0, s0), (c1, s1), (c2, s2), (c3, s3) = after
    left[...] = left_matrix([after[2]] * 3 + [after[1]] * 4, jnp.ones_like(c1))
    right[...] = right_matrix([after[0]] * 7, power(c3, 4) * power(c2, 4) * power(c1, 3))
    made = [before[2][1] / before[2][0], before[3][1] / before[3][0], s1 / c1, s2 / c2, s3 / c3]
    for k, row in enumerate([*made, angle_ref[1:2]]):
        rows[k] = jnp.broadcast_to(row, (8, LANES))


def first_kernel(turn_hbm, angle_hbm, wave_ref, level_ref, out_ref, later_left, later_right, later_rows, turn_ref, angle_ref, wave, left, right,
                 odd, re_sign, im_sign, small_sem, wave_sem, level_sem):
    steps = STEPS
    per = BLOCKS // steps

    def wave_copy(i):
        return pltpu.make_async_copy(
            wave_ref.at[:, pl.ds(i * per, per)], wave.at[i], wave_sem.at[i]
        )

    def level_copy(i):
        return pltpu.make_async_copy(
            level_ref.at[pl.ds(i * per * 8, per * 8)],
            out_ref.at[pl.ds(i * per * 8, per * 8), pl.ds(2 * CHUNK, CHUNK)],
            level_sem.at[i],
        )

    turn_copy = pltpu.make_async_copy(turn_hbm, turn_ref, small_sem.at[0])
    angle_copy = pltpu.make_async_copy(angle_hbm, angle_ref, small_sem.at[1])
    turn_copy.start()
    angle_copy.start()
    for i in range(steps):
        level_copy(i).start()
        wave_copy(i).start()

    set_phases(odd, re_sign, im_sign, ROWS, 7, False)
    turn_copy.wait()
    angle_copy.wait()
    parts = angle_parts(turn_ref, 0)
    (c0, s0), (c1, s1), (c2, s2), (c3, s3) = parts
    left[...] = left_matrix([parts[1]] * 7, jnp.ones_like(c1))
    right[...] = right_matrix([parts[0]] * 7, power(c2, 7) * power(c3, 4))
    later_tables(parts, angle_parts(turn_ref, 1), angle_ref, later_left, later_right, later_rows)
    angle = angle_ref[0:1]
    elsewhere = device_bits()

    @pl.loop(0, steps)
    def _(i):
        level_copy(i).wait()
        wave_copy(i).wait()
        for j in range(per):
            b = i * per + j
            k = (elsewhere + count_bits(b, 4)) & 3
            level = out_ref[pl.ds(b * 8, 8), pl.ds(2 * CHUNK, CHUNK)].reshape(ROWS, LANES)
            co, si = cos_sin(level * angle)
            re, im = wave[i, 0, j], wave[i, 1, j]
            swap = odd[k] > 0.5
            u = jnp.where(swap, im, re) * re_sign[k]
            v = jnp.where(swap, re, im) * im_sign[k]
            re, im = mix_rows_lanes(u * co + v * si, v * co - u * si, left[...], right[...])
            out_ref[pl.ds(b * 8, 8), pl.ds(0, CHUNK)] = re.reshape(8, CHUNK, LANES)
            out_ref[pl.ds(b * 8, 8), pl.ds(CHUNK, CHUNK)] = im.reshape(8, CHUNK, LANES)

    t2 = jnp.broadcast_to(s2 / c2, (8, LANES))

    mix_major(out_ref, out_ref, lambda k, at: k * 8 + at, [t2] * 4)


def middle_kernel(rows, left, right, in_ref, out_ref, held):
    angle, t2 = rows[5, 0:1], rows[0, 0:1]
    mix_major(in_ref, held, lambda k, at: at * 16 + k, [rows[1]] * 4)

    @pl.loop(0, 16 // LOWS)
    def _(i):
        for j in range(LOWS):
            low = i * LOWS + j
            at = [h * 16 + low for h in range(8)]
            re = butterflies([held[k, pl.ds(0, CHUNK)] for k in at], [t2] * 3)
            im = butterflies([held[k, pl.ds(CHUNK, CHUNK)] for k in at], [t2] * 3)
            turned = []
            for h in range(8):
                co, si = cos_sin(in_ref[at[h], pl.ds(2 * CHUNK, CHUNK)] * angle)
                turned.append((re[h] * co + im[h] * si, im[h] * co - re[h] * si))
            re, im = (jnp.concatenate(part, 0) for part in zip(*turned))
            re, im = mix_rows_lanes(re, im, left[...], right[...])
            for h in range(8):
                held[at[h], pl.ds(0, CHUNK)] = re[h * CHUNK : (h + 1) * CHUNK]
                held[at[h], pl.ds(CHUNK, CHUNK)] = im[h * CHUNK : (h + 1) * CHUNK]

    mix_major(held, out_ref, lambda k, at: at * 16 + k, [rows[4]] * 4)


def last_kernel(rows, in_ref, out_ref, held, done, odd, re_sign, im_sign, sem):
    t1, t2 = rows[2], rows[3]
    set_phases(odd, re_sign, im_sign, CHUNK, 4, True)
    elsewhere = device_bits()

    def out_copy(half, b):
        return pltpu.make_async_copy(
            done.at[:, b, :, half], out_ref.at[:, b, :, half], sem.at[half, b]
        )

    for half in range(2):
        re_rows, im_rows = pl.ds(half * 8, 8), pl.ds(CHUNK + half * 8, 8)

        @pl.loop(0, 4)
        def _(i):
            for j in range(2):
                for tile in (re_rows, im_rows):
                    at = i * 2 + j
                    values = [in_ref[b * 8 + at, tile] for b in range(BLOCKS)]
                    for b, value in enumerate(butterflies(values, [t2] * 4)):
                        held[b * 8 + at, tile] = value

        @pl.loop(0, BLOCKS // 2)
        def _(i):
            for j in range(2):
                b = i * 2 + j
                base = elsewhere + count_bits(b, 4)
                re = butterflies([held[b * 8 + r, re_rows] for r in range(8)], [t1] * 3)
                im = butterflies([held[b * 8 + r, im_rows] for r in range(8)], [t1] * 3)
                for r in range(8):
                    k = (base + r.bit_count()) & 3
                    swap = odd[k, re_rows] > 0.5
                    done[0, b, r, half] = jnp.where(swap, im[r], re[r]) * re_sign[k, re_rows]
                    done[1, b, r, half] = jnp.where(swap, re[r], im[r]) * im_sign[k, re_rows]
            for j in range(2):
                out_copy(half, i * 2 + j).start()

    for half in range(2):

        @pl.loop(0, BLOCKS)
        def _(b):
            out_copy(half, b).wait()


LIMIT = pltpu.CompilerParams(vmem_limit_bytes=20 << 20)


def spec(space):
    return pl.BlockSpec(memory_space=space)


def on_device(wave_parts, level_table, diagonal_angles, turn_angles):
    vmem, hbm = spec(pltpu.VMEM), spec(pltpu.HBM)
    square = (256, 256)
    sent, left, right, rows = pl.pallas_call(
        first_kernel,
        name="first",
        compiler_params=LIMIT,
        out_shape=[
            jax.ShapeDtypeStruct((DEVICES, 3 * CHUNK, LANES), F32),
            jax.ShapeDtypeStruct(square, BF16),
            jax.ShapeDtypeStruct(square, BF16),
            jax.ShapeDtypeStruct((6, 8, LANES), F32),
        ],
        in_specs=[hbm] * 4,
        out_specs=[vmem] * 4,
        scratch_shapes=[
            pltpu.SMEM((2, 4), F32),
            pltpu.VMEM((2, LANES), F32),
            pltpu.VMEM((STEPS, 2, BLOCKS // STEPS, ROWS, LANES), F32),
            pltpu.VMEM(square, BF16),
            pltpu.VMEM(square, BF16),
            *[pltpu.VMEM((4, ROWS, LANES), F32)] * 3,
            pltpu.SemaphoreType.DMA((2,)),
            pltpu.SemaphoreType.DMA((STEPS,)),
            pltpu.SemaphoreType.DMA((STEPS,)),
        ],
    )(
        *(
            pltpu.with_memory_space_constraint(x, pltpu.HBM)
            for x in (
                turn_angles,
                diagonal_angles,
                wave_parts,
                level_table.reshape(DEVICES, CHUNK, LANES),
            )
        )
    )
    held = lax.all_to_all(sent, HIGH_LOW, 0, 0, tiled=True)
    sent = pl.pallas_call(
        middle_kernel,
        name="middle",
        compiler_params=LIMIT,
        out_shape=jax.ShapeDtypeStruct((DEVICES, 2 * CHUNK, LANES), F32),
        in_specs=[vmem] * 4,
        out_specs=vmem,
        scratch_shapes=[pltpu.VMEM((DEVICES, 2 * CHUNK, LANES), F32)],
    )(rows, left, right, held)
    held = lax.all_to_all(sent, HIGH_LOW, 0, 0, tiled=True)
    tiled = (2, BLOCKS, 8, 2, 8, LANES)
    out = pl.pallas_call(
        last_kernel,
        name="last",
        compiler_params=LIMIT,
        out_shape=jax.ShapeDtypeStruct(tiled, F32),
        in_specs=[vmem] * 2,
        out_specs=hbm,
        scratch_shapes=[
            pltpu.VMEM((DEVICES, 2 * CHUNK, LANES), F32),
            pltpu.VMEM(tiled, F32),
            *[pltpu.VMEM((4, CHUNK, LANES), F32)] * 3,
            pltpu.SemaphoreType.DMA((2, BLOCKS)),
        ],
    )(rows, held)
    return out.reshape(2, BLOCKS, ROWS, LANES)


def solution(mesh):
    placed = (P(None, HIGH_LOW, None, None), P(HIGH_LOW, None, None), P(), P())
    return jax.shard_map(
        on_device,
        mesh=mesh,
        in_specs=placed,
        out_specs=P(None, HIGH_LOW, None, None),
        check_vma=False,
    )
```

```python
import jax
import jax.numpy as jnp
from jax import lax
from jax.experimental import pallas as pl
from jax.experimental.pallas import tpu as pltpu
from jax.sharding import PartitionSpec as P

HIGH_LOW = ("high", "low")
DEVICES = 128
BLOCKS = 16
ROWS = 128
LANES = 128
LOWS = 16
STEPS = 1
CHUNK = 16
F32 = jnp.float32
BF16 = jnp.bfloat16

COS = (0.9999999403953552, -0.4999995529651642, 0.04166578873991966,
       -0.0013882378116250038, 2.4582879632362165e-05, -2.4136278398145805e-07)
SIN = (1.0, -0.16666662693023682, 0.008333264850080013,
       -0.0001983620022656396, 2.7387263799028005e-06, -2.2399454735477775e-08)


def poly(coefficients, z):
    total = coefficients[-1] * z + coefficients[-2]
    for c in coefficients[-3::-1]:
        total = total * z + c
    return total


def cos_sin(x):
    z = x * x
    return poly(COS, z), x * poly(SIN, z)


def angle_parts(turn_ref, layer):
    return [cos_sin(jnp.full((1, LANES), turn_ref[layer, g], F32)) for g in range(4)]


def power(x, n):
    total = x
    for _ in range(n - 1):
        total = total * x
    return total


def rotation(parts, scale, transposed):
    row = lax.broadcasted_iota(jnp.int32, (128, 128), 0)
    col = lax.broadcasted_iota(jnp.int32, (128, 128), 1)
    out, come = (col, row) if transposed else (row, col)
    total = jnp.broadcast_to(scale, (128, 128))
    for k, (c, s) in enumerate(parts):
        place = 1 << (6 - k)
        same = ((out ^ come) & place) == 0
        signed = jnp.where((out & place) != 0, -s, s)
        total = total * jnp.where(same, c, signed)
    return total


def split(x):
    top = x.astype(BF16)
    return top, (x - top.astype(F32)).astype(BF16)


def left_matrix(parts, scale):
    top, rest = split(rotation(parts, scale, False))
    zero = jnp.zeros_like(top)
    return jnp.concatenate(
        [jnp.concatenate([top, top], 1), jnp.concatenate([rest, zero], 1)], 0
    )


def right_matrix(parts, scale):
    top, rest = split(rotation(parts, scale, True))
    zero = jnp.zeros_like(top)
    return jnp.concatenate(
        [jnp.concatenate([top, rest], 1), jnp.concatenate([top, zero], 1)], 0
    )


def mix_rows_lanes(re, im, left, right):
    re_top, re_rest = split(re)
    im_top, im_rest = split(im)
    block = jnp.concatenate(
        [jnp.concatenate([re_top, im_top], 1), jnp.concatenate([re_rest, im_rest], 1)], 0
    )
    both = jnp.dot(left, block, preferred_element_type=F32)
    both = both[:128] + both[128:]
    re_top, re_rest = split(both[:, :128])
    im_top, im_rest = split(both[:, 128:])
    block = jnp.concatenate(
        [jnp.concatenate([re_top, re_rest], 1), jnp.concatenate([im_top, im_rest], 1)], 0
    )
    both = jnp.dot(block, right, preferred_element_type=F32)
    both = both[:, :128] + both[:, 128:]
    return both[:128], both[128:]


def butterflies(values, tangents):
    values = list(values)
    for k, t in enumerate(tangents):
        apart = len(values) >> (k + 1)
        for i in range(len(values)):
            if not i & apart:
                u, v = values[i], values[i + apart]
                values[i], values[i + apart] = u + t * v, v - t * u
    return values


def count_bits(x, bits):
    total = x & 1
    for k in range(1, bits):
        total = total + ((x >> k) & 1)
    return total


def turned(u, v, c, s):
    return c * u + s * v, c * v - s * u


def two_bits(u):
    return u[1] + u[2], u[3] - u[0], u[0] + u[3], u[1] - u[2]


def two_bits_back(p, m, q, n):
    return q - m, p + n, p - n, q + m


def double_angles(c, s):
    c2, s2 = 1 - 2 * s * s, 2 * s * c
    return c2, s2, 0.5 - s2 * s2, s2 * c2


def mix_four(values, angles):
    c2, s2, half_c4, half_s4 = angles
    rows = [two_bits(values[i : i + 4]) for i in range(0, 16, 4)]
    p, m, q, n = (list(two_bits(column)) for column in zip(*rows))
    for part in (q, n):
        part[0], part[1] = turned(part[0], part[1], c2, s2)
    for k in (2, 3):
        p[k], m[k] = turned(p[k], m[k], c2, s2)
    pp, mm, qq, nn = two_bits((p[0], p[1], m[0], m[1]))
    pp, mm = turned(pp, mm, half_c4, half_s4)
    p[0], p[1], m[0], m[1] = two_bits_back(pp, mm, 0.5 * qq, 0.5 * nn)
    columns = [two_bits_back(*part) for part in (p, m, q, n)]
    return [u for row in zip(*columns) for u in two_bits_back(*row)]


def mix_major(take, put, place, angles):
    @pl.loop(0, 8)
    def _(at):
        for row in range(0, 32, 8):
            tile = pl.ds(row, 8)
            values = [take[place(k, at), tile] for k in range(16)]
            for k, value in enumerate(mix_four(values, angles)):
                put[place(k, at), tile] = value


def device_bits():
    return count_bits(lax.axis_index("high"), 3) + count_bits(lax.axis_index("low"), 4)


def set_phases(odd_ref, re_sign_ref, im_sign_ref, rows, low_rows, back):
    row = lax.broadcasted_iota(jnp.int32, (rows, LANES), 0)
    lane = lax.broadcasted_iota(jnp.int32, (rows, LANES), 1)
    bits = count_bits(row, low_rows) + count_bits(lane, 7)
    for k in range(4):
        p = (bits + k) & 3
        odd_ref[k] = (p & 1).astype(F32)
        plus, minus = (1 - (p & 2)).astype(F32), (1 - ((p + 1) & 2)).astype(F32)
        re_sign_ref[k] = minus if back else plus
        im_sign_ref[k] = plus if back else minus


def later_tables(before, after, angle_ref, left, right, rows):
    (c0, s0), (c1, s1), (c2, s2), (c3, s3) = after
    left[...] = left_matrix([after[2]] * 3 + [after[1]] * 4, jnp.ones_like(c1))
    right[...] = right_matrix([after[0]] * 7, power(c1, 3) / 16)
    made = [angle_ref[1:2], before[2][1] / before[2][0], s1 / c1]
    for c, s in (before[3], after[3], after[2]):
        made.extend(double_angles(c, s))
    for k, row in enumerate(made):
        rows[k] = jnp.broadcast_to(row, (8, LANES))


def first_kernel(turn_hbm, angle_hbm, wave_ref, level_ref, out_ref, later_left, later_right, later_rows, turn_ref, angle_ref, wave, left, right,
                 levels, cosines, sines, odd, re_sign, im_sign, small_sem, wave_sem):
    steps = STEPS
    per = BLOCKS // steps

    def wave_copy(i):
        return pltpu.make_async_copy(
            wave_ref.at[:, pl.ds(i * per, per)], wave.at[i], wave_sem.at[i]
        )

    level_copy = pltpu.make_async_copy(
        level_ref, levels, small_sem.at[2]
    )
    turn_copy = pltpu.make_async_copy(turn_hbm, turn_ref, small_sem.at[0])
    angle_copy = pltpu.make_async_copy(angle_hbm, angle_ref, small_sem.at[1])
    turn_copy.start()
    angle_copy.start()
    level_copy.start()
    set_phases(odd, re_sign, im_sign, ROWS, 7, True)
    wave_copy(0).start()
    turn_copy.wait()
    angle_copy.wait()
    parts = angle_parts(turn_ref, 0)
    (c0, s0), (c1, s1), (c2, s2), (c3, s3) = parts
    left[...] = left_matrix([parts[1]] * 7, jnp.ones_like(c1))
    right[...] = right_matrix([parts[0]] * 7, power(c2, 3) / 16)
    later_tables(parts, angle_parts(turn_ref, 1), angle_ref, later_left, later_right, later_rows)
    for i in range(1, steps):
        wave_copy(i).start()
    angle = angle_ref[0:1]
    elsewhere = device_bits()
    level_copy.wait()

    @pl.loop(0, BLOCKS // 2)
    def _(i):
        for j in range(2):
            b = i * 2 + j
            k = (elsewhere + count_bits(b, 4)) & 3
            level = levels[pl.ds(b * 8, 8)]
            out_ref[pl.ds(b * 8, 8), pl.ds(2 * CHUNK, CHUNK)] = level
            co, si = cos_sin(level.reshape(ROWS, LANES) * angle)
            swap = odd[k] > 0.5
            cosines[b] = jnp.where(swap, si, co) * re_sign[k]
            sines[b] = jnp.where(swap, co, si) * im_sign[k]

    @pl.loop(0, steps)
    def _(i):
        wave_copy(i).wait()
        for j in range(per):
            b = i * per + j
            re, im, co, si = wave[i, 0, j], wave[i, 1, j], cosines[b], sines[b]
            re, im = mix_rows_lanes(re * co + im * si, im * co - re * si, left[...], right[...])
            out_ref[pl.ds(b * 8, 8), pl.ds(0, CHUNK)] = re.reshape(8, CHUNK, LANES)
            out_ref[pl.ds(b * 8, 8), pl.ds(CHUNK, CHUNK)] = im.reshape(8, CHUNK, LANES)

    angles = [jnp.broadcast_to(row, (8, LANES)) for row in double_angles(c2, s2)]
    mix_major(out_ref, out_ref, lambda k, at: k * 8 + at, angles)


def middle_kernel(rows, left, right, in_ref, out_ref, held):
    angle, t2 = rows[0, 0:1], rows[1, 0:1]
    mix_major(in_ref, held, lambda k, at: at * 16 + k, [rows[k] for k in range(3, 7)])

    @pl.loop(0, 16 // LOWS)
    def _(i):
        for j in range(LOWS):
            low = i * LOWS + j
            at = [h * 16 + low for h in range(8)]
            re = butterflies([held[k, pl.ds(0, CHUNK)] for k in at], [t2] * 3)
            im = butterflies([held[k, pl.ds(CHUNK, CHUNK)] for k in at], [t2] * 3)
            phased = []
            for h in range(8):
                co, si = cos_sin(in_ref[at[h], pl.ds(2 * CHUNK, CHUNK)] * angle)
                phased.append((re[h] * co + im[h] * si, im[h] * co - re[h] * si))
            re, im = (jnp.concatenate(part, 0) for part in zip(*phased))
            re, im = mix_rows_lanes(re, im, left[...], right[...])
            for h in range(8):
                held[at[h], pl.ds(0, CHUNK)] = re[h * CHUNK : (h + 1) * CHUNK]
                held[at[h], pl.ds(CHUNK, CHUNK)] = im[h * CHUNK : (h + 1) * CHUNK]

    mix_major(held, out_ref, lambda k, at: at * 16 + k, [rows[k] for k in range(7, 11)])


def last_kernel(rows, in_ref, out_ref, held, done, odd, re_sign, im_sign, sem):
    t1, angles = rows[2], [rows[k] for k in range(11, 15)]
    set_phases(odd, re_sign, im_sign, CHUNK, 4, True)
    elsewhere = device_bits()

    def out_copy(half, b):
        return pltpu.make_async_copy(
            done.at[:, pl.ds(b * 4, 4), :, half],
            out_ref.at[:, pl.ds(b * 4, 4), :, half],
            sem.at[half, b],
        )

    for half in range(2):
        re_rows, im_rows = pl.ds(half * 8, 8), pl.ds(CHUNK + half * 8, 8)

        @pl.loop(0, 4)
        def _(i):
            for j in range(2):
                for tile in (re_rows, im_rows):
                    at = i * 2 + j
                    values = [in_ref[b * 8 + at, tile] for b in range(BLOCKS)]
                    for b, value in enumerate(mix_four(values, angles)):
                        held[b * 8 + at, tile] = value

        @pl.loop(0, BLOCKS // 4)
        def _(i):
            for j in range(4):
                b = i * 4 + j
                base = elsewhere + count_bits(b, 4)
                re = butterflies([held[b * 8 + r, re_rows] for r in range(8)], [t1] * 3)
                im = butterflies([held[b * 8 + r, im_rows] for r in range(8)], [t1] * 3)
                for r in range(8):
                    k = (base + r.bit_count()) & 3
                    swap = odd[k, re_rows] > 0.5
                    done[0, b, r, half] = jnp.where(swap, im[r], re[r]) * re_sign[k, re_rows]
                    done[1, b, r, half] = jnp.where(swap, re[r], im[r]) * im_sign[k, re_rows]
            out_copy(half, i).start()

    for half in range(2):

        for b in range(BLOCKS // 4):
            out_copy(half, b).wait()


LIMIT = pltpu.CompilerParams(vmem_limit_bytes=20 << 20)


def spec(space):
    return pl.BlockSpec(memory_space=space)


def on_device(wave_parts, level_table, diagonal_angles, turn_angles):
    vmem, hbm = spec(pltpu.VMEM), spec(pltpu.HBM)
    square = (256, 256)
    sent, left, right, rows = pl.pallas_call(
        first_kernel,
        name="first",
        compiler_params=LIMIT,
        out_shape=[
            jax.ShapeDtypeStruct((DEVICES, 3 * CHUNK, LANES), F32),
            jax.ShapeDtypeStruct(square, BF16),
            jax.ShapeDtypeStruct(square, BF16),
            jax.ShapeDtypeStruct((15, 8, LANES), F32),
        ],
        in_specs=[hbm] * 4,
        out_specs=[vmem] * 4,
        scratch_shapes=[
            pltpu.SMEM((2, 4), F32),
            pltpu.VMEM((2, LANES), F32),
            pltpu.VMEM((STEPS, 2, BLOCKS // STEPS, ROWS, LANES), F32),
            pltpu.VMEM(square, BF16),
            pltpu.VMEM(square, BF16),
            pltpu.VMEM((DEVICES, CHUNK, LANES), F32),
            *[pltpu.VMEM((BLOCKS, ROWS, LANES), F32)] * 2,
            *[pltpu.VMEM((4, ROWS, LANES), F32)] * 3,
            pltpu.SemaphoreType.DMA((3,)),
            pltpu.SemaphoreType.DMA((STEPS,)),
        ],
    )(
        *(
            pltpu.with_memory_space_constraint(x, pltpu.HBM)
            for x in (
                turn_angles,
                diagonal_angles,
                wave_parts,
                level_table.reshape(DEVICES, CHUNK, LANES),
            )
        )
    )
    held = lax.all_to_all(sent, HIGH_LOW, 0, 0, tiled=True)
    sent = pl.pallas_call(
        middle_kernel,
        name="middle",
        compiler_params=LIMIT,
        out_shape=jax.ShapeDtypeStruct((DEVICES, 2 * CHUNK, LANES), F32),
        in_specs=[vmem] * 4,
        out_specs=vmem,
        scratch_shapes=[pltpu.VMEM((DEVICES, 2 * CHUNK, LANES), F32)],
    )(rows, left, right, held)
    held = lax.all_to_all(sent, HIGH_LOW, 0, 0, tiled=True)
    tiled = (2, BLOCKS, 8, 2, 8, LANES)
    out = pl.pallas_call(
        last_kernel,
        name="last",
        compiler_params=LIMIT,
        out_shape=jax.ShapeDtypeStruct(tiled, F32),
        in_specs=[vmem] * 2,
        out_specs=hbm,
        scratch_shapes=[
            pltpu.VMEM((DEVICES, 2 * CHUNK, LANES), F32),
            pltpu.VMEM(tiled, F32),
            *[pltpu.VMEM((4, CHUNK, LANES), F32)] * 3,
            pltpu.SemaphoreType.DMA((2, BLOCKS // 4)),
        ],
    )(rows, held)
    return out.reshape(2, BLOCKS, ROWS, LANES)


def solution(mesh):
    placed = (P(None, HIGH_LOW, None, None), P(HIGH_LOW, None, None), P(), P())
    return jax.shard_map(
        on_device,
        mesh=mesh,
        in_specs=placed,
        out_specs=P(None, HIGH_LOW, None, None),
        check_vma=False,
    )
```

```python
import jax
import jax.numpy as jnp
from jax import lax
from jax.experimental import pallas as pl
from jax.experimental.pallas import tpu as pltpu
from jax.sharding import PartitionSpec as P

HIGH_LOW = ("high", "low")
DEVICES = 128
BLOCKS = 16
ROWS = 128
LANES = 128
LOWS = 16
STEPS = 1
CHUNK = 16
F32 = jnp.float32
BF16 = jnp.bfloat16

COS = (0.9999999403953552, -0.4999995529651642, 0.04166578873991966,
       -0.0013882378116250038, 2.4582879632362165e-05, -2.4136278398145805e-07)
SIN = (1.0, -0.16666662693023682, 0.008333264850080013,
       -0.0001983620022656396, 2.7387263799028005e-06, -2.2399454735477775e-08)


def poly(coefficients, z):
    total = coefficients[-1] * z + coefficients[-2]
    for c in coefficients[-3::-1]:
        total = total * z + c
    return total


def cos_sin(x):
    z = x * x
    return poly(COS, z), x * poly(SIN, z)


def angle_parts(turn_ref, layer):
    return [cos_sin(jnp.broadcast_to(turn_ref[layer : layer + 1, g : g + 1], (1, LANES))) for g in range(4)]


def power(x, n):
    total = x
    for _ in range(n - 1):
        total = total * x
    return total


def rotation(parts, scale, transposed):
    row = lax.broadcasted_iota(jnp.int32, (128, 128), 0)
    col = lax.broadcasted_iota(jnp.int32, (128, 128), 1)
    out, come = (col, row) if transposed else (row, col)
    total = jnp.broadcast_to(scale, (128, 128))
    for k, (c, s) in enumerate(parts):
        place = 1 << (6 - k)
        same = ((out ^ come) & place) == 0
        signed = jnp.where((out & place) != 0, -s, s)
        total = total * jnp.where(same, c, signed)
    return total


def split(x):
    top = x.astype(BF16)
    return top, (x - top.astype(F32)).astype(BF16)


def left_matrix(parts, scale):
    top, rest = split(rotation(parts, scale, False))
    zero = jnp.zeros_like(top)
    return jnp.concatenate(
        [jnp.concatenate([top, top], 1), jnp.concatenate([rest, zero], 1)], 0
    )


def right_matrix(parts, scale):
    top, rest = split(rotation(parts, scale, True))
    zero = jnp.zeros_like(top)
    return jnp.concatenate(
        [jnp.concatenate([top, rest], 1), jnp.concatenate([top, zero], 1)], 0
    )


def mix_rows_lanes(re, im, left, right):
    re_top, re_rest = split(re)
    im_top, im_rest = split(im)
    block = jnp.concatenate(
        [jnp.concatenate([re_top, im_top], 1), jnp.concatenate([re_rest, im_rest], 1)], 0
    )
    both = jnp.dot(left, block, preferred_element_type=F32)
    both = both[:128] + both[128:]
    re_top, re_rest = split(both[:, :128])
    im_top, im_rest = split(both[:, 128:])
    block = jnp.concatenate(
        [jnp.concatenate([re_top, re_rest], 1), jnp.concatenate([im_top, im_rest], 1)], 0
    )
    both = jnp.dot(block, right, preferred_element_type=F32)
    both = both[:, :128] + both[:, 128:]
    return both[:128], both[128:]


def butterflies(values, tangents):
    values = list(values)
    for k, t in enumerate(tangents):
        apart = len(values) >> (k + 1)
        for i in range(len(values)):
            if not i & apart:
                u, v = values[i], values[i + apart]
                values[i], values[i + apart] = u + t * v, v - t * u
    return values


def count_bits(x, bits):
    total = x & 1
    for k in range(1, bits):
        total = total + ((x >> k) & 1)
    return total


def turned(u, v, c, s):
    return c * u + s * v, c * v - s * u


def two_bits(u):
    return u[1] + u[2], u[3] - u[0], u[0] + u[3], u[1] - u[2]


def two_bits_back(p, m, q, n):
    return q - m, p + n, p - n, q + m


def double_angles(c, s):
    c2, s2 = 1 - 2 * s * s, 2 * s * c
    return c2, s2, 0.5 - s2 * s2, s2 * c2


def mix_four(values, angles):
    c2, s2, half_c4, half_s4 = angles
    rows = [two_bits(values[i : i + 4]) for i in range(0, 16, 4)]
    p, m, q, n = (list(two_bits(column)) for column in zip(*rows))
    for part in (q, n):
        part[0], part[1] = turned(part[0], part[1], c2, s2)
    for k in (2, 3):
        p[k], m[k] = turned(p[k], m[k], c2, s2)
    pp, mm, qq, nn = two_bits((p[0], p[1], m[0], m[1]))
    pp, mm = turned(pp, mm, half_c4, half_s4)
    p[0], p[1], m[0], m[1] = two_bits_back(pp, mm, 0.5 * qq, 0.5 * nn)
    columns = [two_bits_back(*part) for part in (p, m, q, n)]
    return [u for row in zip(*columns) for u in two_bits_back(*row)]


def mix_major(take, put, place, angles):
    @pl.loop(0, 8)
    def _(at):
        for row in range(0, 32, 8):
            tile = pl.ds(row, 8)
            values = [take[place(k, at), tile] for k in range(16)]
            for k, value in enumerate(mix_four(values, angles)):
                put[place(k, at), tile] = value


def device_bits():
    return count_bits(lax.axis_index("high"), 3) + count_bits(lax.axis_index("low"), 4)


def set_phases(odd_ref, re_sign_ref, im_sign_ref, rows, low_rows, back):
    row = lax.broadcasted_iota(jnp.int32, (rows, LANES), 0)
    lane = lax.broadcasted_iota(jnp.int32, (rows, LANES), 1)
    bits = count_bits(row, low_rows) + count_bits(lane, 7)
    for k in range(4):
        p = (bits + k) & 3
        odd_ref[k] = (p & 1).astype(F32)
        plus, minus = (1 - (p & 2)).astype(F32), (1 - ((p + 1) & 2)).astype(F32)
        re_sign_ref[k] = minus if back else plus
        im_sign_ref[k] = plus if back else minus


def later_tables(before, after, angle_ref, left, right, rows):
    (c0, s0), (c1, s1), (c2, s2), (c3, s3) = after
    left[...] = left_matrix([after[2]] * 3 + [after[1]] * 4, jnp.ones_like(c1))
    right[...] = right_matrix([after[0]] * 7, power(c1, 3) / 16)
    made = [angle_ref[1:2], before[2][1] / before[2][0], s1 / c1]
    for c, s in (before[3], after[3], after[2]):
        made.extend(double_angles(c, s))
    for k, row in enumerate(made):
        rows[k] = jnp.broadcast_to(row, (8, LANES))


def first_kernel(turn_hbm, angle_hbm, wave_ref, level_ref, out_ref, later_left, later_right, later_rows, turn_ref, angle_ref, wave, left, right,
                 levels, cosines, sines, odd, re_sign, im_sign, small_sem, wave_sem):
    steps = STEPS
    per = BLOCKS // steps

    def wave_copy(i):
        return pltpu.make_async_copy(
            wave_ref.at[:, pl.ds(i * per, per)], wave.at[i], wave_sem.at[i]
        )

    level_copy = pltpu.make_async_copy(
        level_ref, levels, small_sem.at[2]
    )
    turn_copy = pltpu.make_async_copy(turn_hbm, turn_ref, small_sem.at[0])
    angle_copy = pltpu.make_async_copy(angle_hbm, angle_ref, small_sem.at[1])
    turn_copy.start()
    angle_copy.start()
    level_copy.start()
    set_phases(odd, re_sign, im_sign, ROWS, 7, True)
    wave_copy(0).start()
    turn_copy.wait()
    angle_copy.wait()
    parts = angle_parts(turn_ref, 0)
    (c0, s0), (c1, s1), (c2, s2), (c3, s3) = parts
    left[...] = left_matrix([parts[1]] * 7, jnp.ones_like(c1))
    right[...] = right_matrix([parts[0]] * 7, power(c2, 3) / 16)
    later_tables(parts, angle_parts(turn_ref, 1), angle_ref, later_left, later_right, later_rows)
    for i in range(1, steps):
        wave_copy(i).start()
    angle = angle_ref[0:1]
    elsewhere = device_bits()
    level_copy.wait()

    @pl.loop(0, BLOCKS // 2)
    def _(i):
        for j in range(2):
            b = i * 2 + j
            k = (elsewhere + count_bits(b, 4)) & 3
            level = levels[pl.ds(b * 8, 8)]
            out_ref[pl.ds(b * 8, 8), pl.ds(2 * CHUNK, CHUNK)] = level
            co, si = cos_sin(level.reshape(ROWS, LANES) * angle)
            swap = odd[k] > 0.5
            cosines[b] = jnp.where(swap, si, co) * re_sign[k]
            sines[b] = jnp.where(swap, co, si) * im_sign[k]

    @pl.loop(0, steps)
    def _(i):
        wave_copy(i).wait()
        for j in range(per):
            b = i * per + j
            re, im, co, si = wave[i, 0, j], wave[i, 1, j], cosines[b], sines[b]
            re, im = mix_rows_lanes(re * co + im * si, im * co - re * si, left[...], right[...])
            out_ref[pl.ds(b * 8, 8), pl.ds(0, CHUNK)] = re.reshape(8, CHUNK, LANES)
            out_ref[pl.ds(b * 8, 8), pl.ds(CHUNK, CHUNK)] = im.reshape(8, CHUNK, LANES)

    angles = [jnp.broadcast_to(row, (8, LANES)) for row in double_angles(c2, s2)]
    mix_major(out_ref, out_ref, lambda k, at: k * 8 + at, angles)


def middle_kernel(rows, left, right, in_ref, out_ref, held):
    angle, t2 = rows[0, 0:1], rows[1, 0:1]
    mix_major(in_ref, held, lambda k, at: at * 16 + k, [rows[k] for k in range(3, 7)])

    @pl.loop(0, 16 // LOWS)
    def _(i):
        for j in range(LOWS):
            low = i * LOWS + j
            at = [h * 16 + low for h in range(8)]
            re = butterflies([held[k, pl.ds(0, CHUNK)] for k in at], [t2] * 3)
            im = butterflies([held[k, pl.ds(CHUNK, CHUNK)] for k in at], [t2] * 3)
            phased = []
            for h in range(8):
                co, si = cos_sin(in_ref[at[h], pl.ds(2 * CHUNK, CHUNK)] * angle)
                phased.append((re[h] * co + im[h] * si, im[h] * co - re[h] * si))
            re, im = (jnp.concatenate(part, 0) for part in zip(*phased))
            re, im = mix_rows_lanes(re, im, left[...], right[...])
            for h in range(8):
                held[at[h], pl.ds(0, CHUNK)] = re[h * CHUNK : (h + 1) * CHUNK]
                held[at[h], pl.ds(CHUNK, CHUNK)] = im[h * CHUNK : (h + 1) * CHUNK]

    mix_major(held, out_ref, lambda k, at: at * 16 + k, [rows[k] for k in range(7, 11)])


def last_kernel(rows, in_ref, out_ref, held, done, odd, re_sign, im_sign, sem):
    t1, angles = rows[2], [rows[k] for k in range(11, 15)]
    set_phases(odd, re_sign, im_sign, CHUNK, 4, True)
    elsewhere = device_bits()

    def out_copy(half, b):
        return pltpu.make_async_copy(
            done.at[:, pl.ds(b * 4, 4), :, half],
            out_ref.at[:, pl.ds(b * 4, 4), :, half],
            sem.at[half, b],
        )

    for half in range(2):
        re_rows, im_rows = pl.ds(half * 8, 8), pl.ds(CHUNK + half * 8, 8)

        @pl.loop(0, 4)
        def _(i):
            for j in range(2):
                for tile in (re_rows, im_rows):
                    at = i * 2 + j
                    values = [in_ref[b * 8 + at, tile] for b in range(BLOCKS)]
                    for b, value in enumerate(mix_four(values, angles)):
                        held[b * 8 + at, tile] = value

        @pl.loop(0, BLOCKS // 4)
        def _(i):
            for j in range(4):
                b = i * 4 + j
                base = elsewhere + count_bits(b, 4)
                re = butterflies([held[b * 8 + r, re_rows] for r in range(8)], [t1] * 3)
                im = butterflies([held[b * 8 + r, im_rows] for r in range(8)], [t1] * 3)
                for r in range(8):
                    k = (base + r.bit_count()) & 3
                    swap = odd[k, re_rows] > 0.5
                    done[0, b, r, half] = jnp.where(swap, im[r], re[r]) * re_sign[k, re_rows]
                    done[1, b, r, half] = jnp.where(swap, re[r], im[r]) * im_sign[k, re_rows]
            out_copy(half, i).start()

    for half in range(2):

        for b in range(BLOCKS // 4):
            out_copy(half, b).wait()


LIMIT = pltpu.CompilerParams(vmem_limit_bytes=20 << 20)


def spec(space):
    return pl.BlockSpec(memory_space=space)


def on_device(wave_parts, level_table, diagonal_angles, turn_angles):
    vmem, hbm = spec(pltpu.VMEM), spec(pltpu.HBM)
    square = (256, 256)
    sent, left, right, rows = pl.pallas_call(
        first_kernel,
        name="first",
        compiler_params=LIMIT,
        out_shape=[
            jax.ShapeDtypeStruct((DEVICES, 3 * CHUNK, LANES), F32),
            jax.ShapeDtypeStruct(square, BF16),
            jax.ShapeDtypeStruct(square, BF16),
            jax.ShapeDtypeStruct((15, 8, LANES), F32),
        ],
        in_specs=[hbm] * 4,
        out_specs=[vmem] * 4,
        scratch_shapes=[
            pltpu.VMEM((2, 4), F32),
            pltpu.VMEM((2, LANES), F32),
            pltpu.VMEM((STEPS, 2, BLOCKS // STEPS, ROWS, LANES), F32),
            pltpu.VMEM(square, BF16),
            pltpu.VMEM(square, BF16),
            pltpu.VMEM((DEVICES, CHUNK, LANES), F32),
            *[pltpu.VMEM((BLOCKS, ROWS, LANES), F32)] * 2,
            *[pltpu.VMEM((4, ROWS, LANES), F32)] * 3,
            pltpu.SemaphoreType.DMA((3,)),
            pltpu.SemaphoreType.DMA((STEPS,)),
        ],
    )(
        *(
            pltpu.with_memory_space_constraint(x, pltpu.HBM)
            for x in (
                turn_angles,
                diagonal_angles,
                wave_parts,
                level_table.reshape(DEVICES, CHUNK, LANES),
            )
        )
    )
    held = lax.all_to_all(sent, HIGH_LOW, 0, 0, tiled=True)
    sent = pl.pallas_call(
        middle_kernel,
        name="middle",
        compiler_params=LIMIT,
        out_shape=jax.ShapeDtypeStruct((DEVICES, 2 * CHUNK, LANES), F32),
        in_specs=[vmem] * 4,
        out_specs=vmem,
        scratch_shapes=[pltpu.VMEM((DEVICES, 2 * CHUNK, LANES), F32)],
    )(rows, left, right, held)
    held = lax.all_to_all(sent, HIGH_LOW, 0, 0, tiled=True)
    tiled = (2, BLOCKS, 8, 2, 8, LANES)
    out = pl.pallas_call(
        last_kernel,
        name="last",
        compiler_params=LIMIT,
        out_shape=jax.ShapeDtypeStruct(tiled, F32),
        in_specs=[vmem] * 2,
        out_specs=hbm,
        scratch_shapes=[
            pltpu.VMEM((DEVICES, 2 * CHUNK, LANES), F32),
            pltpu.VMEM(tiled, F32),
            *[pltpu.VMEM((4, CHUNK, LANES), F32)] * 3,
            pltpu.SemaphoreType.DMA((2, BLOCKS // 4)),
        ],
    )(rows, held)
    return out.reshape(2, BLOCKS, ROWS, LANES)


def solution(mesh):
    placed = (P(None, HIGH_LOW, None, None), P(HIGH_LOW, None, None), P(), P())
    return jax.shard_map(
        on_device,
        mesh=mesh,
        in_specs=placed,
        out_specs=P(None, HIGH_LOW, None, None),
        check_vma=False,
    )
```

```python
import jax
import jax.numpy as jnp
from jax import lax
from jax.experimental import pallas as pl
from jax.experimental.pallas import tpu as pltpu
from jax.sharding import PartitionSpec as P

HIGH_LOW = ("high", "low")
DEVICES = 128
BLOCKS = 16
ROWS = 128
LANES = 128
LOWS = 16
STEPS = 1
CHUNK = 16
F32 = jnp.float32
BF16 = jnp.bfloat16

COS = (0.9999999403953552, -0.4999995529651642, 0.04166578873991966,
       -0.0013882378116250038, 2.4582879632362165e-05, -2.4136278398145805e-07)
SIN = (1.0, -0.16666662693023682, 0.008333264850080013,
       -0.0001983620022656396, 2.7387263799028005e-06, -2.2399454735477775e-08)


def poly(coefficients, z):
    total = coefficients[-1] * z + coefficients[-2]
    for c in coefficients[-3::-1]:
        total = total * z + c
    return total


def cos_sin(x):
    z = x * x
    return poly(COS, z), x * poly(SIN, z)


def angle_parts(turn_ref, layer):
    return [cos_sin(jnp.full((1, LANES), turn_ref[layer, g], F32)) for g in range(4)]


def power(x, n):
    total = x
    for _ in range(n - 1):
        total = total * x
    return total


def rotation(parts, scale, transposed):
    row = lax.broadcasted_iota(jnp.int32, (128, 128), 0)
    col = lax.broadcasted_iota(jnp.int32, (128, 128), 1)
    out, come = (col, row) if transposed else (row, col)
    total = jnp.broadcast_to(scale, (128, 128))
    for k, (c, s) in enumerate(parts):
        place = 1 << (6 - k)
        same = ((out ^ come) & place) == 0
        signed = jnp.where((out & place) != 0, -s, s)
        total = total * jnp.where(same, c, signed)
    return total


def split(x):
    top = x.astype(BF16)
    return top, (x - top.astype(F32)).astype(BF16)


def left_matrix(parts, scale):
    top, rest = split(rotation(parts, scale, False))
    zero = jnp.zeros_like(top)
    return jnp.concatenate(
        [jnp.concatenate([top, top], 1), jnp.concatenate([rest, zero], 1)], 0
    )


def right_matrix(parts, scale):
    top, rest = split(rotation(parts, scale, True))
    zero = jnp.zeros_like(top)
    return jnp.concatenate(
        [jnp.concatenate([top, rest], 1), jnp.concatenate([top, zero], 1)], 0
    )


def mix_rows_lanes(re, im, left, right):
    re_top, re_rest = split(re)
    im_top, im_rest = split(im)
    block = jnp.concatenate(
        [jnp.concatenate([re_top, im_top], 1), jnp.concatenate([re_rest, im_rest], 1)], 0
    )
    both = jnp.dot(left, block, preferred_element_type=F32)
    both = both[:128] + both[128:]
    re_top, re_rest = split(both[:, :128])
    im_top, im_rest = split(both[:, 128:])
    block = jnp.concatenate(
        [jnp.concatenate([re_top, re_rest], 1), jnp.concatenate([im_top, im_rest], 1)], 0
    )
    both = jnp.dot(block, right, preferred_element_type=F32)
    both = both[:, :128] + both[:, 128:]
    return both[:128], both[128:]


def butterflies(values, tangents):
    values = list(values)
    for k, t in enumerate(tangents):
        apart = len(values) >> (k + 1)
        for i in range(len(values)):
            if not i & apart:
                u, v = values[i], values[i + apart]
                values[i], values[i + apart] = u + t * v, v - t * u
    return values


def count_bits(x, bits):
    total = x & 1
    for k in range(1, bits):
        total = total + ((x >> k) & 1)
    return total


def turned(u, v, c, s):
    return c * u + s * v, c * v - s * u


def two_bits(u):
    return u[1] + u[2], u[3] - u[0], u[0] + u[3], u[1] - u[2]


def two_bits_back(p, m, q, n):
    return q - m, p + n, p - n, q + m


def double_angles(c, s):
    c2, s2 = 1 - 2 * s * s, 2 * s * c
    return c2, s2, 0.5 - s2 * s2, s2 * c2


def mix_four(values, angles):
    c2, s2, half_c4, half_s4 = angles
    rows = [two_bits(values[i : i + 4]) for i in range(0, 16, 4)]
    p, m, q, n = (list(two_bits(column)) for column in zip(*rows))
    for part in (q, n):
        part[0], part[1] = turned(part[0], part[1], c2, s2)
    for k in (2, 3):
        p[k], m[k] = turned(p[k], m[k], c2, s2)
    pp, mm, qq, nn = two_bits((p[0], p[1], m[0], m[1]))
    pp, mm = turned(pp, mm, half_c4, half_s4)
    p[0], p[1], m[0], m[1] = two_bits_back(pp, mm, 0.5 * qq, 0.5 * nn)
    columns = [two_bits_back(*part) for part in (p, m, q, n)]
    return [u for row in zip(*columns) for u in two_bits_back(*row)]


def mix_major(take, put, place, angles):
    @pl.loop(0, 8)
    def _(at):
        for row in range(0, 32, 8):
            tile = pl.ds(row, 8)
            values = [take[place(k, at), tile] for k in range(16)]
            for k, value in enumerate(mix_four(values, angles)):
                put[place(k, at), tile] = value


def device_bits():
    return count_bits(lax.axis_index("high"), 3) + count_bits(lax.axis_index("low"), 4)


def set_phases(odd_ref, re_sign_ref, im_sign_ref, rows, low_rows, back):
    row = lax.broadcasted_iota(jnp.int32, (rows, LANES), 0)
    lane = lax.broadcasted_iota(jnp.int32, (rows, LANES), 1)
    bits = count_bits(row, low_rows) + count_bits(lane, 7)
    for k in range(4):
        p = (bits + k) & 3
        odd_ref[k] = (p & 1).astype(F32)
        plus, minus = (1 - (p & 2)).astype(F32), (1 - ((p + 1) & 2)).astype(F32)
        re_sign_ref[k] = minus if back else plus
        im_sign_ref[k] = plus if back else minus


def later_tables(before, after, angle_ref, left, right, rows):
    (c0, s0), (c1, s1), (c2, s2), (c3, s3) = after
    left[...] = left_matrix([after[2]] * 3 + [after[1]] * 4, jnp.ones_like(c1))
    right[...] = right_matrix([after[0]] * 7, power(c1, 3) / 16)
    made = [angle_ref[1:2], before[2][1] / before[2][0], s1 / c1]
    for c, s in (before[3], after[3], after[2]):
        made.extend(double_angles(c, s))
    for k, row in enumerate(made):
        rows[k] = jnp.broadcast_to(row, (8, LANES))


def first_kernel(turn_hbm, angle_hbm, wave_ref, level_ref, out_ref, later_left, later_right, later_rows, turn_ref, angle_ref, wave, left, right,
                 levels, cosines, sines, odd, re_sign, im_sign, small_sem, wave_sem):
    steps = STEPS
    per = BLOCKS // steps

    def wave_copy(i):
        return pltpu.make_async_copy(
            wave_ref.at[:, pl.ds(i * per, per)], wave.at[i], wave_sem.at[i]
        )

    def level_copy(i):
        part = pl.ds(i * 64, 64)
        return pltpu.make_async_copy(level_ref.at[part], levels.at[part], small_sem.at[2 + i])

    turn_copy = pltpu.make_async_copy(turn_hbm, turn_ref, small_sem.at[0])
    angle_copy = pltpu.make_async_copy(angle_hbm, angle_ref, small_sem.at[1])
    turn_copy.start()
    angle_copy.start()
    level_copy(0).start()
    level_copy(1).start()
    set_phases(odd, re_sign, im_sign, ROWS, 7, True)
    wave_copy(0).start()
    turn_copy.wait()
    angle_copy.wait()
    parts = angle_parts(turn_ref, 0)
    (c0, s0), (c1, s1), (c2, s2), (c3, s3) = parts
    left[...] = left_matrix([parts[1]] * 7, jnp.ones_like(c1))
    right[...] = right_matrix([parts[0]] * 7, power(c2, 3) / 16)
    for i in range(1, steps):
        wave_copy(i).start()
    angle = angle_ref[0:1]
    elsewhere = device_bits()
    for half in range(2):
        level_copy(half).wait()

        @pl.loop(0, BLOCKS // 4)
        def _(i):
            for j in range(2):
                b = half * 8 + i * 2 + j
                k = (elsewhere + count_bits(b, 4)) & 3
                level = levels[pl.ds(b * 8, 8)]
                out_ref[pl.ds(b * 8, 8), pl.ds(2 * CHUNK, CHUNK)] = level
                co, si = cos_sin(level.reshape(ROWS, LANES) * angle)
                swap = odd[k] > 0.5
                cosines[b] = jnp.where(swap, si, co) * re_sign[k]
                sines[b] = jnp.where(swap, co, si) * im_sign[k]

    @pl.loop(0, steps)
    def _(i):
        wave_copy(i).wait()
        later_tables(parts, angle_parts(turn_ref, 1), angle_ref, later_left, later_right, later_rows)
        for j in range(per):
            b = i * per + j
            re, im, co, si = wave[i, 0, j], wave[i, 1, j], cosines[b], sines[b]
            re, im = mix_rows_lanes(re * co + im * si, im * co - re * si, left[...], right[...])
            out_ref[pl.ds(b * 8, 8), pl.ds(0, CHUNK)] = re.reshape(8, CHUNK, LANES)
            out_ref[pl.ds(b * 8, 8), pl.ds(CHUNK, CHUNK)] = im.reshape(8, CHUNK, LANES)

    angles = [jnp.broadcast_to(row, (8, LANES)) for row in double_angles(c2, s2)]
    mix_major(out_ref, out_ref, lambda k, at: k * 8 + at, angles)


def middle_kernel(rows, left, right, in_ref, out_ref, held):
    angle, t2 = rows[0, 0:1], rows[1, 0:1]
    mix_major(in_ref, held, lambda k, at: at * 16 + k, [rows[k] for k in range(3, 7)])

    @pl.loop(0, 16 // LOWS)
    def _(i):
        for j in range(LOWS):
            low = i * LOWS + j
            at = [h * 16 + low for h in range(8)]
            re = butterflies([held[k, pl.ds(0, CHUNK)] for k in at], [t2] * 3)
            im = butterflies([held[k, pl.ds(CHUNK, CHUNK)] for k in at], [t2] * 3)
            phased = []
            for h in range(8):
                co, si = cos_sin(in_ref[at[h], pl.ds(2 * CHUNK, CHUNK)] * angle)
                phased.append((re[h] * co + im[h] * si, im[h] * co - re[h] * si))
            re, im = (jnp.concatenate(part, 0) for part in zip(*phased))
            re, im = mix_rows_lanes(re, im, left[...], right[...])
            for h in range(8):
                held[at[h], pl.ds(0, CHUNK)] = re[h * CHUNK : (h + 1) * CHUNK]
                held[at[h], pl.ds(CHUNK, CHUNK)] = im[h * CHUNK : (h + 1) * CHUNK]

    mix_major(held, out_ref, lambda k, at: at * 16 + k, [rows[k] for k in range(7, 11)])


def last_kernel(rows, in_ref, out_ref, held, done, odd, re_sign, im_sign, sem):
    t1, angles = rows[2], [rows[k] for k in range(11, 15)]
    set_phases(odd, re_sign, im_sign, CHUNK, 4, True)
    elsewhere = device_bits()

    def out_copy(half, b):
        return pltpu.make_async_copy(
            done.at[:, pl.ds(b * 4, 4), :, half],
            out_ref.at[:, pl.ds(b * 4, 4), :, half],
            sem.at[half, b],
        )

    for half in range(2):
        re_rows, im_rows = pl.ds(half * 8, 8), pl.ds(CHUNK + half * 8, 8)

        @pl.loop(0, 4)
        def _(i):
            for j in range(2):
                for tile in (re_rows, im_rows):
                    at = i * 2 + j
                    values = [in_ref[b * 8 + at, tile] for b in range(BLOCKS)]
                    for b, value in enumerate(mix_four(values, angles)):
                        held[b * 8 + at, tile] = value

        @pl.loop(0, BLOCKS // 4)
        def _(i):
            for j in range(4):
                b = i * 4 + j
                base = elsewhere + count_bits(b, 4)
                re = butterflies([held[b * 8 + r, re_rows] for r in range(8)], [t1] * 3)
                im = butterflies([held[b * 8 + r, im_rows] for r in range(8)], [t1] * 3)
                for r in range(8):
                    k = (base + r.bit_count()) & 3
                    swap = odd[k, re_rows] > 0.5
                    done[0, b, r, half] = jnp.where(swap, im[r], re[r]) * re_sign[k, re_rows]
                    done[1, b, r, half] = jnp.where(swap, re[r], im[r]) * im_sign[k, re_rows]
            out_copy(half, i).start()

    for half in range(2):

        for b in range(BLOCKS // 4):
            out_copy(half, b).wait()


LIMIT = pltpu.CompilerParams(vmem_limit_bytes=20 << 20)


def spec(space):
    return pl.BlockSpec(memory_space=space)


def on_device(wave_parts, level_table, diagonal_angles, turn_angles):
    vmem, hbm = spec(pltpu.VMEM), spec(pltpu.HBM)
    square = (256, 256)
    sent, left, right, rows = pl.pallas_call(
        first_kernel,
        name="first",
        compiler_params=LIMIT,
        out_shape=[
            jax.ShapeDtypeStruct((DEVICES, 3 * CHUNK, LANES), F32),
            jax.ShapeDtypeStruct(square, BF16),
            jax.ShapeDtypeStruct(square, BF16),
            jax.ShapeDtypeStruct((15, 8, LANES), F32),
        ],
        in_specs=[hbm] * 4,
        out_specs=[vmem] * 4,
        scratch_shapes=[
            pltpu.SMEM((2, 4), F32),
            pltpu.VMEM((2, LANES), F32),
            pltpu.VMEM((STEPS, 2, BLOCKS // STEPS, ROWS, LANES), F32),
            pltpu.VMEM(square, BF16),
            pltpu.VMEM(square, BF16),
            pltpu.VMEM((DEVICES, CHUNK, LANES), F32),
            *[pltpu.VMEM((BLOCKS, ROWS, LANES), F32)] * 2,
            *[pltpu.VMEM((4, ROWS, LANES), F32)] * 3,
            pltpu.SemaphoreType.DMA((4,)),
            pltpu.SemaphoreType.DMA((STEPS,)),
        ],
    )(
        *(
            pltpu.with_memory_space_constraint(x, pltpu.HBM)
            for x in (
                turn_angles,
                diagonal_angles,
                wave_parts,
                level_table.reshape(DEVICES, CHUNK, LANES),
            )
        )
    )
    held = lax.all_to_all(sent, HIGH_LOW, 0, 0, tiled=True)
    sent = pl.pallas_call(
        middle_kernel,
        name="middle",
        compiler_params=LIMIT,
        out_shape=jax.ShapeDtypeStruct((DEVICES, 2 * CHUNK, LANES), F32),
        in_specs=[vmem] * 4,
        out_specs=vmem,
        scratch_shapes=[pltpu.VMEM((DEVICES, 2 * CHUNK, LANES), F32)],
    )(rows, left, right, held)
    held = lax.all_to_all(sent, HIGH_LOW, 0, 0, tiled=True)
    tiled = (2, BLOCKS, 8, 2, 8, LANES)
    out = pl.pallas_call(
        last_kernel,
        name="last",
        compiler_params=LIMIT,
        out_shape=jax.ShapeDtypeStruct(tiled, F32),
        in_specs=[vmem] * 2,
        out_specs=hbm,
        scratch_shapes=[
            pltpu.VMEM((DEVICES, 2 * CHUNK, LANES), F32),
            pltpu.VMEM(tiled, F32),
            *[pltpu.VMEM((4, CHUNK, LANES), F32)] * 3,
            pltpu.SemaphoreType.DMA((2, BLOCKS // 4)),
        ],
    )(rows, held)
    return out.reshape(2, BLOCKS, ROWS, LANES)


def solution(mesh):
    placed = (P(None, HIGH_LOW, None, None), P(HIGH_LOW, None, None), P(), P())
    return jax.shard_map(
        on_device,
        mesh=mesh,
        in_specs=placed,
        out_specs=P(None, HIGH_LOW, None, None),
        check_vma=False,
    )
```
